256 devices in a mesh: band: 8 (over y_lo, x), ga: 32 (over z, y_hi, core).
Axes of the slice: x: 4, y: 4 (y_hi: 2, y_lo: 2; y = y_hi * 2 + y_lo), z: 8, core: 2. Of those that a mesh axis runs over, the one named last changes fastest.
Arguments:
- wavefunctions: bfloat16 [1024, 98304], P('band', 'ga'), may hold values from -6 to 6
- projectors: bfloat16 [2048, 98304], P('band', 'ga'), may hold values from -0.125 to 0.125
- kinetic_diag: float32 [98304], P('ga'), may hold values from 0.1 to 4
- species_index: int32 [256], replicated, may hold values from 0 to 3
- coupling: float32 [4, 8, 8], replicated, may hold values from -5 to 5
Outputs:
- applied: bfloat16 [1024, 98304], P('band', 'ga')
The draws below stay inside these ranges and needn't reach their ends.
All inputs are finite; a program needn't handle non-finite values.
Results may differ from the reference program's by a relative error of at most 0.015.
Values may be sent and summed in bfloat16 or wider, within the bound.
A program may use at most 64 MiB of HBM per device.

```python
import math
import jax
import jax.numpy as jnp
from jax import lax

NG = 98304
NPA = 8
ATOMS = 256
NSPEC = 4
BANDS = 1024
NPROJ = 2048


def place_ends(array, rng, low, top_value):
    longest = array.shape.index(max(array.shape))
    spots = []
    for shift in (0, 1):
        where = [jax.random.randint(jax.random.fold_in(rng, axis), (), 0, length) for axis, length in enumerate(array.shape)]
        where[longest] = (where[longest] + shift) % array.shape[longest]
        spots.append(tuple(where))
    return array.at[spots[0]].set(low).at[spots[1]].set(top_value)


def shard_levels(rng, extent, split, smallest, largest):
    def one(axis_at, shards_of):
        steps = jax.random.uniform(jax.random.fold_in(jax.random.fold_in(rng, 6), axis_at), (shards_of,), jnp.float32, smallest / len(split), largest / len(split))
        return jnp.repeat(jnp.exp(steps), extent[axis_at] // shards_of).reshape((-1,) + (1,) * (len(extent) - axis_at - 1))

    gain = one(*split[0])
    for cut in split[1:]:
        gain = gain * one(*cut)
    return gain


def noise(rng, dims, spread, reach, shards=(), held_as=jnp.bfloat16):
    values = spread * jax.random.normal(rng, dims, jnp.float32)
    if shards:
        values = values * shard_levels(rng, dims, shards, -0.22, 0.18)
    return jnp.clip(values, -reach, reach).astype(held_as)


def setup_inputs(seed: int = 0) -> dict:
    splits = jax.random.split(jax.random.key(seed), 6)
    return {
        "wavefunctions": noise(splits[0], (BANDS, NG), 1.0, 6.0, ((0, 8), (1, 32))),
        "projectors": noise(splits[1], (NPROJ, NG), ((NG * NPROJ) ** -0.25), 0.125, ((0, 8), (1, 32))),
        "kinetic_diag": jnp.clip(jnp.exp(math.log(4.0) - 3.6888794 * jax.random.uniform(splits[2], (NG,), jnp.float32) ** shard_levels(splits[2], (NG,), ((0, 32),), -0.2, 0.2)), 0.1, 4.0),
        "species_index": place_ends(jax.random.randint(splits[3], (ATOMS,), 0, NSPEC), jax.random.fold_in(splits[3], 1), 0, NSPEC - 1).astype(jnp.int32),
        "coupling": noise(splits[4], (NSPEC, NPA, NPA), 0.35, 5.0, (), jnp.float32),
    }


def reference(wavefunctions, projectors, kinetic_diag, species_index, coupling):
    correlations = jnp.dot(wavefunctions, projectors.T, preferred_element_type=jnp.float32)
    onehot = (species_index[:, None] == jnp.arange(NSPEC, dtype=jnp.int32)[None, :]).astype(jnp.float32)
    blocks = jnp.einsum("as,sij->aij", onehot, coupling, precision=lax.Precision.HIGHEST)
    mixed = jnp.einsum("baj,aij->bai", correlations.reshape(BANDS, ATOMS, NPA), blocks, precision=lax.Precision.HIGHEST)
    mixed = mixed.reshape(BANDS, NPROJ).astype(jnp.bfloat16)
    nonlocal_term = jnp.dot(mixed, projectors, preferred_element_type=jnp.float32)
    return (kinetic_diag[None, :] * wavefunctions.astype(jnp.float32) + nonlocal_term).astype(jnp.bfloat16)
```

```python
import functools

import jax
import jax.numpy as jnp
from jax import lax
from jax.experimental import pallas as pl
from jax.experimental.pallas import tpu as pltpu
from jax.sharding import PartitionSpec as P

NPA = 8
NX = 4
NZ = 8
MESH = pl.DeviceIdType.MESH
CUTS = ((0, 384), (384, 128))
W0R, W1R, W1L, W0L, FR, FL, P0, P1 = range(8)
RSY, AGY, RSZ, AGZ = 8, 10, 12, 14
T2A, T2B, RB, LA, ACA, ACB = range(16, 22)
COPIES = 22


def kernel(
    w_hbm,
    p_hbm,
    kin_ref,
    mt_ref,
    out_ref,
    wbuf,
    pbuf,
    c0,
    c1,
    r0,
    r1,
    sums,
    ysend,
    yrecv,
    dpair,
    dall,
    part_send,
    part_recv,
    own,
    block_diag,
    send_sem,
    recv_sem,
    load_sem,
):
    band = lax.axis_index("band")
    ga = lax.axis_index("ga")
    rows, cols = w_hbm.shape
    prows = p_hbm.shape[0]
    half_rows = rows // 2
    half = cols // 2
    x = lax.rem(band, NX)
    y_lo = band // NX
    core = lax.rem(ga, 2)
    y_hi = lax.rem(ga // 2, 2)
    z = ga // 4
    peer = z * 2 + core
    right = (y_lo * NX + lax.rem(x + 1, NX), ga)
    left = (y_lo * NX + lax.rem(x + NX - 1, NX), ga)
    across = ((1 - y_lo) * NX + x, ga)
    far = (band, (z * 2 + 1 - y_hi) * 2 + core)
    npeers = NZ * 2

    def peer_device(k):
        q = lax.rem(peer + k, npeers)
        return q, (band, ((q // 2) * 2 + y_hi) * 2 + lax.rem(q, 2))

    def copy(index, src, dst, device):
        return pltpu.make_async_remote_copy(
            src_ref=src,
            dst_ref=dst,
            send_sem=send_sem.at[index],
            recv_sem=recv_sem.at[index],
            device_id=device,
            device_id_type=MESH,
        )

    load_w = pltpu.make_async_copy(w_hbm, wbuf.at[pl.ds(0, rows)], load_sem.at[0])
    load_p = pltpu.make_async_copy(p_hbm, pbuf.at[pl.ds(0, prows)], load_sem.at[1])
    load_w.start()
    load_p.start()

    barrier = pltpu.get_barrier_semaphore()
    for device in (right, left, across, far):
        pl.semaphore_signal(barrier, inc=1, device_id=device, device_id_type=MESH)

    @pl.loop(1, npeers)
    def _(k):
        _, device = peer_device(k)
        pl.semaphore_signal(barrier, inc=1, device_id=device, device_id_type=MESH)

    pl.semaphore_wait(barrier, 4 + npeers - 1)

    low, high = pl.ds(0, half_rows), pl.ds(half_rows, half_rows)
    wrow = lambda block, part: pl.ds(block * rows + part * half_rows, half_rows)
    p0 = copy(P0, p_hbm.at[pl.ds(0, prows // 2)], pbuf.at[pl.ds(prows, prows // 2)], across)
    p1 = copy(
        P1,
        p_hbm.at[pl.ds(prows // 2, prows // 2)],
        pbuf.at[pl.ds(prows + prows // 2, prows // 2)],
        across,
    )
    w0r = copy(W0R, w_hbm.at[low], wbuf.at[wrow(1, 0)], right)
    w1r = copy(W1R, w_hbm.at[high], wbuf.at[wrow(1, 1)], right)
    w1l = copy(W1L, w_hbm.at[high], wbuf.at[wrow(2, 1)], left)
    w0l = copy(W0L, w_hbm.at[low], wbuf.at[wrow(2, 0)], left)
    fr = copy(FR, wbuf.at[wrow(1, 0)], wbuf.at[wrow(3, 0)], right)
    fl = copy(FL, wbuf.at[wrow(2, 1)], wbuf.at[wrow(3, 1)], left)
    for c in (w0r, w1l, p0, w1r, w0l, p1):
        c.start()

    starts = (
        band * prows,
        band * prows + 128,
        across[0] * prows,
        across[0] * prows + 128,
    )
    q_at = lax.broadcasted_iota(jnp.int32, (128, 128), 0) // NPA
    p_at = lax.broadcasted_iota(jnp.int32, (128, 128), 1) // NPA
    for b, start in enumerate(starts):
        strip = mt_ref[:, pl.ds(pl.multiple_of(start, 128), 128)]
        tiled = jnp.concatenate([strip] * (128 // NPA), axis=0)
        block_diag[pl.ds(b * 128, 128), :] = jnp.where(q_at == p_at, tiled, 0.0)

    cbuf, rbuf = (c0, c1), (r0, r1)

    def correlate(row, count, pstart, pcount, target, tcol):
        c = lax.dot_general(
            wbuf[pl.ds(row, count), :],
            pbuf[pl.ds(pstart, pcount), :],
            (((1,), (1,)), ((), ())),
            preferred_element_type=jnp.float32,
        )
        target[pl.ds(row, count), pl.ds(tcol, pcount)] = c.astype(jnp.bfloat16)

    load_w.wait()
    load_p.wait()
    correlate(0, rows, 0, prows, c0, 0)
    w0r.wait_recv()
    fr.start()
    w1l.wait_recv()
    fl.start()
    w1r.wait_recv()
    w0l.wait_recv()
    correlate(rows, 2 * rows, 0, prows, c0, 0)
    p0.wait_recv()
    correlate(0, 3 * rows, prows, prows // 2, c0, prows)
    fr.wait_recv()
    fl.wait_recv()
    correlate(3 * rows, rows, 0, prows + prows // 2, c0, 0)

    share = 4 * rows // npeers
    hshare = share // 2

    def scatter_start(i):
        @pl.loop(1, npeers)
        def _(k):
            q, device = peer_device(k)
            copy(
                RSZ + i,
                cbuf[i].at[pl.ds(pl.multiple_of(q * share, share), share)],
                rbuf[i].at[pl.ds(pl.multiple_of(peer * share, share), share)],
                device,
            ).start()

        here = pl.ds(pl.multiple_of(peer * share, share), share)
        rbuf[i][here, :] = cbuf[i][here, :]

    def many(index, ref):
        return copy(index, ref, ref, right)

    keep = pl.ds(pl.multiple_of(y_hi * hshare, hshare), hshare)
    give = pl.ds(pl.multiple_of((1 - y_hi) * hshare, hshare), hshare)
    rest = pl.ds(0, (npeers - 1) * share)

    def y_sum(i):
        start, width = CUTS[i]
        at = pl.ds(start, width)
        return copy(RSY + i, ysend.at[:, at], yrecv.at[:, at], far)

    def y_share(i):
        start, width = CUTS[i]
        at = pl.ds(start, width)
        return copy(AGY + i, dpair.at[keep, at], dpair.at[keep, at], far)

    def scatter_sum(i):
        start, width = CUTS[i]
        at = pl.ds(start, width)
        many(RSZ + i, rbuf[i].at[rest]).wait_recv()
        total = rbuf[i][pl.ds(0, share), :].astype(jnp.float32)
        for q in range(1, npeers):
            total += rbuf[i][pl.ds(q * share, share), :].astype(jnp.float32)
        sums[:, at] = total
        ysend[:, at] = sums[give, at].astype(jnp.bfloat16)
        y_sum(i).start()

    def couple(i):
        start, width = CUTS[i]
        y_sum(i).wait_recv()
        for b in range(start // 128, (start + width) // 128):
            at = pl.ds(b * 128, 128)
            total = sums[keep, at] + yrecv[:, at].astype(jnp.float32)
            mixed = jnp.dot(
                total,
                block_diag[at, :],
                precision=lax.Precision.HIGHEST,
                preferred_element_type=jnp.float32,
            )
            dpair[keep, at] = mixed.astype(jnp.bfloat16)
        y_share(i).start()

    def gather_start(i):
        start, width = CUTS[i]
        at = pl.ds(start, width)
        y_share(i).wait_recv()
        here = pl.ds(pl.multiple_of(peer * share, share), share)

        @pl.loop(1, npeers)
        def _(k):
            _, device = peer_device(k)
            copy(AGZ + i, dpair.at[:, at], dall.at[here, at], device).start()

        dall[here, at] = dpair[:, at]

    scatter_start(0)
    p1.wait_recv()
    correlate(0, 4 * rows, prows + prows // 2, prows // 2, c1, 0)
    scatter_start(1)
    scatter_sum(0)
    couple(0)
    gather_start(0)
    scatter_sum(1)
    couple(1)
    gather_start(1)
    for i in range(2):
        start, width = CUTS[i]
        many(AGZ + i, dall.at[rest, pl.ds(start, width)]).wait_recv()

    def partial(block, side):
        return jnp.dot(
            dall[pl.ds(block * rows, rows), :],
            pbuf[:, pl.ds(side * half, half)],
            preferred_element_type=jnp.float32,
        )

    def send_part(index, device):
        slot = index - T2A
        return copy(index, part_send.at[slot], part_recv.at[slot], device)

    t2a, t2b = send_part(T2A, right), send_part(T2B, left)
    rb, la = send_part(RB, right), send_part(LA, left)
    aca, acb = send_part(ACA, right), send_part(ACB, left)

    def put(index, value):
        part_send[index - T2A] = value.astype(jnp.bfloat16)

    def got(index):
        return part_recv[index - T2A].astype(jnp.float32)

    put(T2A, partial(3, 0))
    t2a.start()
    put(T2B, partial(3, 1))
    t2b.start()
    put(RB, partial(2, 1))
    rb.start()
    put(LA, partial(1, 0))
    la.start()
    own[:, pl.ds(0, half)] = partial(2, 0)
    own[:, pl.ds(half, half)] = partial(1, 1)
    t2a.wait_recv()
    put(ACA, own[:, pl.ds(0, half)] + got(T2A))
    aca.start()
    t2b.wait_recv()
    put(ACB, own[:, pl.ds(half, half)] + got(T2B))
    acb.start()
    for side in range(2):
        at = pl.ds(side * half, half)
        own[:, at] = partial(0, side) + kin_ref[:, at] * wbuf[pl.ds(0, rows), at].astype(
            jnp.float32
        )
    la.wait_recv()
    own[:, pl.ds(0, half)] += got(LA)
    rb.wait_recv()
    own[:, pl.ds(half, half)] += got(RB)
    aca.wait_recv()
    out_ref[:, pl.ds(0, half)] = (own[:, pl.ds(0, half)] + got(ACA)).astype(jnp.bfloat16)
    acb.wait_recv()
    out_ref[:, pl.ds(half, half)] = (own[:, pl.ds(half, half)] + got(ACB)).astype(jnp.bfloat16)

    for c in (w0r, w1r, w1l, w0l, fr, fl, p0, p1, t2a, t2b, rb, la, aca, acb):
        c.wait_send()
    for i in range(2):
        start, width = CUTS[i]
        y_sum(i).wait_send()
        y_share(i).wait_send()
        many(RSZ + i, rbuf[i].at[rest]).wait_send()
        many(AGZ + i, dall.at[rest, pl.ds(start, width)]).wait_send()


def local(wavefunctions, projectors, kinetic_diag, species_index, coupling):
    rows, cols = wavefunctions.shape
    prows = projectors.shape[0]
    width = 2 * prows
    bf16, f32 = jnp.bfloat16, jnp.float32
    turned = coupling.transpose(0, 2, 1)
    picked = jnp.zeros((NPA, species_index.shape[0], NPA), f32)
    for k in range(coupling.shape[0]):
        picked = jnp.where(
            (species_index == k)[None, :, None], turned[k][:, None, :], picked
        )
    mt = picked.reshape(NPA, species_index.shape[0] * NPA)
    share = 4 * rows // (2 * NZ)
    vmem = pl.BlockSpec(memory_space=pltpu.VMEM)
    anywhere = pl.BlockSpec(memory_space=pl.ANY)
    return pl.pallas_call(
        kernel,
        out_shape=jax.ShapeDtypeStruct((rows, cols), bf16),
        in_specs=[anywhere, anywhere, vmem, vmem],
        out_specs=vmem,
        scratch_shapes=[
            pltpu.VMEM((4 * rows, cols), bf16),
            pltpu.VMEM((width, cols), bf16),
            pltpu.VMEM((4 * rows, CUTS[0][1]), bf16),
            pltpu.VMEM((4 * rows, CUTS[1][1]), bf16),
            pltpu.VMEM((4 * rows, CUTS[0][1]), bf16),
            pltpu.VMEM((4 * rows, CUTS[1][1]), bf16),
            pltpu.VMEM((share, width), f32),
            pltpu.VMEM((share // 2, width), bf16),
            pltpu.VMEM((share // 2, width), bf16),
            pltpu.VMEM((share, width), bf16),
            pltpu.VMEM((4 * rows, width), bf16),
            pltpu.VMEM((6, rows, cols // 2), bf16),
            pltpu.VMEM((6, rows, cols // 2), bf16),
            pltpu.VMEM((rows, cols), f32),
            pltpu.VMEM((width, 128), f32),
            pltpu.SemaphoreType.DMA((COPIES,)),
            pltpu.SemaphoreType.DMA((COPIES,)),
            pltpu.SemaphoreType.DMA((2,)),
        ],
        compiler_params=pltpu.CompilerParams(
            collective_id=0, has_side_effects=True, vmem_limit_bytes=48 * 1024 * 1024
        ),
    )(wavefunctions, projectors, kinetic_diag.reshape(1, cols), mt)


def solution(mesh):
    in_specs = (P("band", "ga"), P("band", "ga"), P("ga"), P(), P())
    out_specs = P("band", "ga")
    return jax.shard_map(local, mesh=mesh, in_specs=in_specs, out_specs=out_specs, check_vma=False)
```

```python
import jax
import jax.numpy as jnp
from jax import lax
from jax.experimental import pallas as pl
from jax.experimental.pallas import tpu as pltpu
from jax.sharding import PartitionSpec as P

NPA = 8
NX = 4
NZ = 8
MESH = pl.DeviceIdType.MESH
CUTS = ((0, 384), (384, 128))
W0R, W1R, W1L, W0L, FR, FL, P0, P1, RS0, RSY, RS1, AG0, AGC, AG1 = range(14)
T2A, T2B, RB, LA, ACA, ACB = range(14, 20)
COPIES = 20
ROUNDS = 4


def kernel(
    w_hbm,
    p_hbm,
    kin_hbm,
    species_hbm,
    coupling_ref,
    out_ref,
    wbuf,
    pbuf,
    c0,
    c1,
    r0,
    r1,
    sums,
    ysend,
    yrecv,
    dall,
    part_send,
    part_recv,
    own,
    block_diag,
    kin_ref,
    species,
    send_sem,
    recv_sem,
    load_sem,
    meet_sem,
):
    band = lax.axis_index("band")
    ga = lax.axis_index("ga")
    rows, cols = w_hbm.shape
    prows = p_hbm.shape[0]
    half_rows = rows // 2
    half = cols // 2
    x = lax.rem(band, NX)
    y_lo = band // NX
    core = lax.rem(ga, 2)
    y_hi = lax.rem(ga // 2, 2)
    z = ga // 4
    right = (y_lo * NX + lax.rem(x + 1, NX), ga)
    left = (y_lo * NX + lax.rem(x + NX - 1, NX), ga)
    across = ((1 - y_lo) * NX + x, ga)

    def at_place(z, y_hi, core):
        return (band, (z * 2 + y_hi) * 2 + core)

    far = at_place(z, 1 - y_hi, core)
    twin = at_place(z, y_hi, 1 - core)
    above = at_place(lax.rem(z + 1, NZ), y_hi, core)
    below = at_place(lax.rem(z + NZ - 1, NZ), y_hi, core)
    nga = 4 * NZ
    npeers = 2 * NZ
    peer = core * NZ + z

    def copy(index, src, dst, device):
        return pltpu.make_async_remote_copy(
            src_ref=src,
            dst_ref=dst,
            send_sem=send_sem.at[index],
            recv_sem=recv_sem.at[index],
            device_id=device,
            device_id_type=MESH,
        )

    load_w = pltpu.make_async_copy(w_hbm, wbuf.at[pl.ds(0, rows)], load_sem.at[0])
    load_p = pltpu.make_async_copy(p_hbm, pbuf.at[pl.ds(0, prows)], load_sem.at[1])
    load_kin = pltpu.make_async_copy(kin_hbm, kin_ref, load_sem.at[2])
    load_species = pltpu.make_async_copy(species_hbm, species, load_sem.at[3])
    for c in (load_species, load_w, load_p, load_kin):
        c.start()

    barrier = pltpu.get_barrier_semaphore()
    near = (right, left, across, far, twin, above, below)
    for device in near:
        pl.semaphore_signal(barrier, inc=1, device_id=device, device_id_type=MESH)
    pl.semaphore_wait(barrier, len(near))

    low, high = pl.ds(0, half_rows), pl.ds(half_rows, half_rows)
    wrow = lambda block, part: pl.ds(block * rows + part * half_rows, half_rows)
    p0 = copy(P0, p_hbm.at[pl.ds(0, prows // 2)], pbuf.at[pl.ds(prows, prows // 2)], across)
    p1 = copy(
        P1,
        p_hbm.at[pl.ds(prows // 2, prows // 2)],
        pbuf.at[pl.ds(prows + prows // 2, prows // 2)],
        across,
    )
    w0r = copy(W0R, w_hbm.at[low], wbuf.at[wrow(1, 0)], right)
    w1r = copy(W1R, w_hbm.at[high], wbuf.at[wrow(1, 1)], right)
    w1l = copy(W1L, w_hbm.at[high], wbuf.at[wrow(2, 1)], left)
    w0l = copy(W0L, w_hbm.at[low], wbuf.at[wrow(2, 0)], left)
    fr = copy(FR, wbuf.at[wrow(1, 0)], wbuf.at[wrow(3, 0)], right)
    fl = copy(FL, wbuf.at[wrow(2, 1)], wbuf.at[wrow(3, 1)], left)
    for c in (w0r, w1l, p0, w1r, w0l, p1):
        c.start()

    load_species.wait()
    lane = lax.broadcasted_iota(jnp.int32, (NPA, 128), 1)
    index_at = lax.broadcasted_iota(jnp.int32, (NPA, 128), 0)
    spread = jnp.where(lax.rem(lane, NPA) == index_at, 1.0, 0.0).astype(jnp.float32)
    turned = [
        lax.dot_general(
            coupling_ref[k],
            spread,
            (((0,), (0,)), ((), ())),
            precision=lax.Precision.HIGHEST,
            preferred_element_type=jnp.float32,
        )
        for k in range(coupling_ref.shape[0])
    ]
    q_at = lax.broadcasted_iota(jnp.int32, (128, 128), 0) // NPA
    p_at = lax.broadcasted_iota(jnp.int32, (128, 128), 1) // NPA
    per_block = 128 // NPA
    atoms = prows // NPA
    for b in range(4):
        first = (band if b < 2 else across[0]) * atoms + (b % 2) * per_block
        kinds = jnp.zeros((NPA, 128), jnp.int32)
        for a in range(per_block):
            kinds = jnp.where(lane // NPA == a, species[first + a], kinds)
        strip = jnp.zeros((NPA, 128), jnp.float32)
        for k, matrix in enumerate(turned):
            strip = jnp.where(kinds == k, matrix, strip)
        tiled = jnp.concatenate([strip] * per_block, axis=0)
        block_diag[pl.ds(b * 128, 128), :] = jnp.where(q_at == p_at, tiled, 0.0)

    for i in range(ROUNDS):
        for device in (above, below):
            pl.semaphore_signal(
                meet_sem.at[i], inc=1, device_id=device, device_id_type=MESH
            )
        pl.semaphore_wait(meet_sem.at[i], 2)
    pl.semaphore_signal(
        meet_sem.at[ROUNDS], inc=1, device_id=twin, device_id_type=MESH
    )
    pl.semaphore_wait(meet_sem.at[ROUNDS], 1)

    def correlate(row, count, pstart, pcount, target, tcol):
        c = lax.dot_general(
            wbuf[pl.ds(row, count), :],
            pbuf[pl.ds(pstart, pcount), :],
            (((1,), (1,)), ((), ())),
            preferred_element_type=jnp.float32,
        )
        target[pl.ds(row, count), pl.ds(tcol, pcount)] = c.astype(jnp.bfloat16)

    share = 4 * rows // npeers
    piece = share // 2
    mine = pl.ds(pl.multiple_of((peer * 2 + y_hi) * piece, piece), piece)
    keep = pl.ds(pl.multiple_of(y_hi * piece, piece), piece)
    give = pl.ds(pl.multiple_of((1 - y_hi) * piece, piece), piece)
    first, last = (pl.ds(*cut) for cut in CUTS)

    def many(index, ref):
        return copy(index, ref, ref, right)

    all_rs0 = many(RS0, r0.at[pl.ds(0, (npeers - 1) * share)])
    all_rs1 = many(RS1, r1.at[pl.ds(0, (nga - 1) * piece)])
    all_ag0 = many(AG0, dall.at[pl.ds(0, (npeers - 1) * piece), first])
    all_ag1 = many(AG1, dall.at[pl.ds(0, (nga - 1) * piece), last])

    def scatter_first(low, count):
        @pl.loop(0, count)
        def _(k):
            q = low + lax.rem(peer + k, count)

            @pl.when(q != peer)
            def _():
                copy(
                    RS0,
                    c0.at[pl.ds(pl.multiple_of(q * share, share), share)],
                    r0.at[pl.ds(pl.multiple_of(peer * share, share), share)],
                    at_place(lax.rem(q, NZ), y_hi, q // NZ),
                ).start()

    def other(k):
        g = lax.rem(ga + k, nga)
        place = (g // 4, lax.rem(g // 2, 2), lax.rem(g, 2))
        row = ((place[2] * NZ + place[0]) * 2 + place[1]) * piece
        return pl.ds(pl.multiple_of(row, piece), piece), at_place(*place)

    def couple(total, b):
        return jnp.dot(
            total,
            block_diag[pl.ds(b * 128, 128), :],
            precision=lax.Precision.HIGHEST,
            preferred_element_type=jnp.float32,
        ).astype(jnp.bfloat16)

    load_w.wait()
    load_p.wait()
    correlate(0, rows, 0, prows, c0, 0)
    w0r.wait_recv()
    fr.start()
    w1l.wait_recv()
    fl.start()
    w1r.wait_recv()
    w0l.wait_recv()
    correlate(rows, 2 * rows, 0, prows, c0, 0)
    p0.wait_recv()
    correlate(0, 3 * rows, prows, prows // 2, c0, prows)
    early = 3 * npeers // 4
    scatter_first(0, early)
    fr.wait_recv()
    fl.wait_recv()
    correlate(3 * rows, rows, 0, prows + prows // 2, c0, 0)
    scatter_first(early, npeers - early)
    here = pl.ds(pl.multiple_of(peer * share, share), share)
    r0[here, :] = c0[here, :]

    p1.wait_recv()
    correlate(0, 4 * rows, prows + prows // 2, prows // 2, c1, 0)

    @pl.loop(1, nga)
    def _(k):
        at, device = other(k)
        copy(RS1, c1.at[at], r1.at[mine], device).start()

    r1[mine, :] = c1[mine, :]

    all_rs0.wait_recv()
    total = r0[pl.ds(0, share), :].astype(jnp.float32)
    for q in range(1, npeers):
        total += r0[pl.ds(q * share, share), :].astype(jnp.float32)
    sums[...] = total
    ysend[...] = sums[give, :].astype(jnp.bfloat16)
    y_sum = copy(RSY, ysend, yrecv, far)
    y_sum.start()
    y_sum.wait_recv()
    for b in range(CUTS[0][1] // 128):
        at = pl.ds(b * 128, 128)
        dall[mine, at] = couple(sums[keep, at] + yrecv[:, at].astype(jnp.float32), b)

    @pl.loop(1, npeers)
    def _(k):
        j = lax.rem(z * 2 + y_hi + k, npeers)
        device = at_place(j // 2, lax.rem(j, 2), core)
        copy(AG0, dall.at[mine, first], dall.at[mine, first], device).start()

    all_rs1.wait_recv()
    total = r1[pl.ds(0, piece), :].astype(jnp.float32)
    for q in range(1, nga):
        total += r1[pl.ds(q * piece, piece), :].astype(jnp.float32)
    dall[mine, last] = couple(total, 3)

    @pl.loop(1, nga)
    def _(k):
        _, device = other(k)
        copy(AG1, dall.at[mine, last], dall.at[mine, last], device).start()

    all_ag0.wait_recv()
    half_block = pl.ds(pl.multiple_of(core * 2 * rows, 2 * rows), 2 * rows)
    to_twin = copy(AGC, dall.at[half_block, first], dall.at[half_block, first], twin)
    to_twin.start()
    to_twin.wait_recv()
    all_ag1.wait_recv()

    def partial(block, side):
        return jnp.dot(
            dall[pl.ds(block * rows, rows), :],
            pbuf[:, pl.ds(side * half, half)],
            preferred_element_type=jnp.float32,
        )

    def send_part(index, device):
        slot = index - T2A
        return copy(index, part_send.at[slot], part_recv.at[slot], device)

    t2a, t2b = send_part(T2A, right), send_part(T2B, left)
    rb, la = send_part(RB, right), send_part(LA, left)
    aca, acb = send_part(ACA, right), send_part(ACB, left)

    def put(index, value):
        part_send[index - T2A] = value.astype(jnp.bfloat16)

    def got(index):
        return part_recv[index - T2A].astype(jnp.float32)

    put(T2A, partial(3, 0))
    t2a.start()
    put(T2B, partial(3, 1))
    t2b.start()
    put(RB, partial(2, 1))
    rb.start()
    put(LA, partial(1, 0))
    la.start()
    own[:, pl.ds(0, half)] = partial(2, 0)
    own[:, pl.ds(half, half)] = partial(1, 1)
    t2a.wait_recv()
    put(ACA, own[:, pl.ds(0, half)] + got(T2A))
    aca.start()
    t2b.wait_recv()
    put(ACB, own[:, pl.ds(half, half)] + got(T2B))
    acb.start()
    load_kin.wait()
    for side in range(2):
        at = pl.ds(side * half, half)
        own[:, at] = partial(0, side) + kin_ref[:, at] * wbuf[pl.ds(0, rows), at].astype(
            jnp.float32
        )
    la.wait_recv()
    own[:, pl.ds(0, half)] += got(LA)
    rb.wait_recv()
    own[:, pl.ds(half, half)] += got(RB)
    aca.wait_recv()
    out_ref[:, pl.ds(0, half)] = (own[:, pl.ds(0, half)] + got(ACA)).astype(jnp.bfloat16)
    acb.wait_recv()
    out_ref[:, pl.ds(half, half)] = (own[:, pl.ds(half, half)] + got(ACB)).astype(jnp.bfloat16)

    for c in (w0r, w1r, w1l, w0l, fr, fl, p0, p1, y_sum, to_twin, t2a, t2b, rb, la, aca, acb):
        c.wait_send()
    for c in (all_rs0, all_rs1, all_ag0, all_ag1):
        c.wait_send()


def local(wavefunctions, projectors, kinetic_diag, species_index, coupling):
    rows, cols = wavefunctions.shape
    prows = projectors.shape[0]
    width = 2 * prows
    bf16, f32 = jnp.bfloat16, jnp.float32
    share = 4 * rows // (2 * NZ)
    vmem = pl.BlockSpec(memory_space=pltpu.VMEM)
    anywhere = pl.BlockSpec(memory_space=pl.ANY)
    return pl.pallas_call(
        kernel,
        out_shape=jax.ShapeDtypeStruct((rows, cols), bf16),
        in_specs=[anywhere, anywhere, anywhere, anywhere, vmem],
        out_specs=vmem,
        scratch_shapes=[
            pltpu.VMEM((4 * rows, cols), bf16),
            pltpu.VMEM((width, cols), bf16),
            pltpu.VMEM((4 * rows, CUTS[0][1]), bf16),
            pltpu.VMEM((4 * rows, CUTS[1][1]), bf16),
            pltpu.VMEM((4 * rows, CUTS[0][1]), bf16),
            pltpu.VMEM((4 * rows, CUTS[1][1]), bf16),
            pltpu.VMEM((share, CUTS[0][1]), f32),
            pltpu.VMEM((share // 2, CUTS[0][1]), bf16),
            pltpu.VMEM((share // 2, CUTS[0][1]), bf16),
            pltpu.VMEM((4 * rows, width), bf16),
            pltpu.VMEM((6, rows, cols // 2), bf16),
            pltpu.VMEM((6, rows, cols // 2), bf16),
            pltpu.VMEM((rows, cols), f32),
            pltpu.VMEM((width, 128), f32),
            pltpu.VMEM((1, cols), f32),
            pltpu.SMEM(species_index.shape, jnp.int32),
            pltpu.SemaphoreType.DMA((COPIES,)),
            pltpu.SemaphoreType.DMA((COPIES,)),
            pltpu.SemaphoreType.DMA((4,)),
            pltpu.SemaphoreType.REGULAR((ROUNDS + 1,)),
        ],
        compiler_params=pltpu.CompilerParams(
            collective_id=0, has_side_effects=True, vmem_limit_bytes=67043328
        ),
    )(wavefunctions, projectors, kinetic_diag.reshape(1, cols), species_index, coupling)


def solution(mesh):
    in_specs = (P("band", "ga"), P("band", "ga"), P("ga"), P(), P())
    out_specs = P("band", "ga")
    return jax.shard_map(local, mesh=mesh, in_specs=in_specs, out_specs=out_specs, check_vma=False)
```

```python
import jax
import jax.numpy as jnp
from jax import lax
from jax.experimental import pallas as pl
from jax.experimental.pallas import tpu as pltpu
from jax.sharding import PartitionSpec as P

NPA = 8
NX = 4
NZ = 8
MESH = pl.DeviceIdType.MESH
CUTS = ((0, 384), (384, 128))
W0R, W1R, W1L, W0L, FR, FL, P0, P1, RS0, RSY, RS1, AG0, AGC, AG1 = range(14)
T2A, T2B, RB, LA, ACA, ACB = range(14, 26, 2)
COPIES = 26
ROUNDS = 4


def kernel(
    w_hbm,
    p_hbm,
    kin_hbm,
    species_hbm,
    coupling_ref,
    out_ref,
    wbuf,
    pbuf,
    c0,
    c1,
    r0,
    r1,
    sums,
    ysend,
    yrecv,
    dall,
    part_send,
    part_recv,
    own,
    block_diag,
    kin_ref,
    species,
    send_sem,
    recv_sem,
    load_sem,
    meet_sem,
):
    band = lax.axis_index("band")
    ga = lax.axis_index("ga")
    rows, cols = w_hbm.shape
    prows = p_hbm.shape[0]
    half_rows = rows // 2
    half = cols // 2
    x = lax.rem(band, NX)
    y_lo = band // NX
    core = lax.rem(ga, 2)
    y_hi = lax.rem(ga // 2, 2)
    z = ga // 4
    right = (y_lo * NX + lax.rem(x + 1, NX), ga)
    left = (y_lo * NX + lax.rem(x + NX - 1, NX), ga)
    across = ((1 - y_lo) * NX + x, ga)

    def at_place(z, y_hi, core):
        return (band, (z * 2 + y_hi) * 2 + core)

    far = at_place(z, 1 - y_hi, core)
    twin = at_place(z, y_hi, 1 - core)
    above = at_place(lax.rem(z + 1, NZ), y_hi, core)
    below = at_place(lax.rem(z + NZ - 1, NZ), y_hi, core)
    nga = 4 * NZ
    npeers = 2 * NZ
    peer = core * NZ + z

    def copy(index, src, dst, device):
        return pltpu.make_async_remote_copy(
            src_ref=src,
            dst_ref=dst,
            send_sem=send_sem.at[index],
            recv_sem=recv_sem.at[index],
            device_id=device,
            device_id_type=MESH,
        )

    load_w = pltpu.make_async_copy(w_hbm, wbuf.at[pl.ds(0, rows)], load_sem.at[0])
    load_p = pltpu.make_async_copy(p_hbm, pbuf.at[pl.ds(0, prows)], load_sem.at[1])
    load_kin = pltpu.make_async_copy(kin_hbm, kin_ref, load_sem.at[2])
    load_species = pltpu.make_async_copy(species_hbm, species, load_sem.at[3])
    for c in (load_species, load_w, load_p, load_kin):
        c.start()

    barrier = pltpu.get_barrier_semaphore()
    near = (right, left, across, far, twin, above, below)
    for device in near:
        pl.semaphore_signal(barrier, inc=1, device_id=device, device_id_type=MESH)
    pl.semaphore_wait(barrier, len(near))

    low, high = pl.ds(0, half_rows), pl.ds(half_rows, half_rows)
    wrow = lambda block, part: pl.ds(block * rows + part * half_rows, half_rows)
    p0 = copy(P0, p_hbm.at[pl.ds(0, prows // 2)], pbuf.at[pl.ds(prows, prows // 2)], across)
    p1 = copy(
        P1,
        p_hbm.at[pl.ds(prows // 2, prows // 2)],
        pbuf.at[pl.ds(prows + prows // 2, prows // 2)],
        across,
    )
    w0r = copy(W0R, w_hbm.at[low], wbuf.at[wrow(1, 0)], right)
    w1r = copy(W1R, w_hbm.at[high], wbuf.at[wrow(1, 1)], right)
    w1l = copy(W1L, w_hbm.at[high], wbuf.at[wrow(2, 1)], left)
    w0l = copy(W0L, w_hbm.at[low], wbuf.at[wrow(2, 0)], left)
    fr = copy(FR, wbuf.at[wrow(1, 0)], wbuf.at[wrow(3, 0)], right)
    fl = copy(FL, wbuf.at[wrow(2, 1)], wbuf.at[wrow(3, 1)], left)
    for c in (w0r, w1l, p0, w1r, w0l, p1):
        c.start()

    load_species.wait()
    lane = lax.broadcasted_iota(jnp.int32, (NPA, 128), 1)
    index_at = lax.broadcasted_iota(jnp.int32, (NPA, 128), 0)
    spread = jnp.where(lax.rem(lane, NPA) == index_at, 1.0, 0.0).astype(jnp.float32)
    turned = [
        lax.dot_general(
            coupling_ref[k],
            spread,
            (((0,), (0,)), ((), ())),
            precision=lax.Precision.HIGHEST,
            preferred_element_type=jnp.float32,
        )
        for k in range(coupling_ref.shape[0])
    ]
    q_at = lax.broadcasted_iota(jnp.int32, (128, 128), 0) // NPA
    p_at = lax.broadcasted_iota(jnp.int32, (128, 128), 1) // NPA
    per_block = 128 // NPA
    atoms = prows // NPA
    for b in range(4):
        first = (band if b < 2 else across[0]) * atoms + (b % 2) * per_block
        kinds = jnp.zeros((NPA, 128), jnp.int32)
        for a in range(per_block):
            kinds = jnp.where(lane // NPA == a, species[first + a], kinds)
        strip = jnp.zeros((NPA, 128), jnp.float32)
        for k, matrix in enumerate(turned):
            strip = jnp.where(kinds == k, matrix, strip)
        tiled = jnp.concatenate([strip] * per_block, axis=0)
        block_diag[pl.ds(b * 128, 128), :] = jnp.where(q_at == p_at, tiled, 0.0)

    for i in range(ROUNDS):
        for device in (above, below):
            pl.semaphore_signal(
                meet_sem.at[i], inc=1, device_id=device, device_id_type=MESH
            )
        pl.semaphore_wait(meet_sem.at[i], 2)
    pl.semaphore_signal(
        meet_sem.at[ROUNDS], inc=1, device_id=twin, device_id_type=MESH
    )
    pl.semaphore_wait(meet_sem.at[ROUNDS], 1)

    def correlate(row, count, pstart, pcount, target, tcol):
        c = lax.dot_general(
            wbuf[pl.ds(row, count), :],
            pbuf[pl.ds(pstart, pcount), :],
            (((1,), (1,)), ((), ())),
            preferred_element_type=jnp.float32,
        )
        target[pl.ds(row, count), pl.ds(tcol, pcount)] = c.astype(jnp.bfloat16)

    share = 4 * rows // npeers
    piece = share // 2
    mine = pl.ds(pl.multiple_of((peer * 2 + y_hi) * piece, piece), piece)
    keep = pl.ds(pl.multiple_of(y_hi * piece, piece), piece)
    give = pl.ds(pl.multiple_of((1 - y_hi) * piece, piece), piece)
    first, last = (pl.ds(*cut) for cut in CUTS)

    def many(index, ref):
        return copy(index, ref, ref, right)

    all_rs0 = many(RS0, r0.at[pl.ds(0, (npeers - 1) * share)])
    all_rs1 = many(RS1, r1.at[pl.ds(0, (nga - 1) * piece)])
    all_ag0 = many(AG0, dall.at[pl.ds(0, (npeers - 1) * piece), first])
    all_ag1 = many(AG1, dall.at[pl.ds(0, (nga - 1) * piece), last])

    def scatter_first(low, count):
        @pl.loop(0, count)
        def _(k):
            q = low + lax.rem(peer + k, count)

            @pl.when(q != peer)
            def _():
                copy(
                    RS0,
                    c0.at[pl.ds(pl.multiple_of(q * share, share), share)],
                    r0.at[pl.ds(pl.multiple_of(peer * share, share), share)],
                    at_place(lax.rem(q, NZ), y_hi, q // NZ),
                ).start()

    def other(k):
        i = k // 4
        d = NZ // 2 + jnp.where(lax.rem(i, 2) == 0, i // 2, -((i + 1) // 2))
        place = (
            lax.rem(z + d, NZ),
            lax.rem(y_hi + 1 - lax.rem(k, 4) // 2, 2),
            lax.rem(core + 1 - lax.rem(k, 2), 2),
        )
        row = ((place[2] * NZ + place[0]) * 2 + place[1]) * piece
        return pl.ds(pl.multiple_of(row, piece), piece), at_place(*place)

    def couple(total, b):
        return jnp.dot(
            total,
            block_diag[pl.ds(b * 128, 128), :],
            precision=lax.Precision.HIGHEST,
            preferred_element_type=jnp.float32,
        ).astype(jnp.bfloat16)

    load_w.wait()
    load_p.wait()
    correlate(0, rows, 0, prows, c0, 0)
    w0r.wait_recv()
    fr.start()
    w1l.wait_recv()
    fl.start()
    w1r.wait_recv()
    w0l.wait_recv()
    correlate(rows, 2 * rows, 0, prows, c0, 0)
    p0.wait_recv()
    correlate(0, 3 * rows, prows, prows // 2, c0, prows)
    early = 3 * npeers // 4
    scatter_first(0, early)
    fr.wait_recv()
    fl.wait_recv()
    correlate(3 * rows, rows, 0, prows + prows // 2, c0, 0)
    scatter_first(early, npeers - early)
    here = pl.ds(pl.multiple_of(peer * share, share), share)
    r0[here, :] = c0[here, :]

    all_rs0.wait_recv()
    total = r0[pl.ds(0, share), :].astype(jnp.float32)
    for q in range(1, npeers):
        total += r0[pl.ds(q * share, share), :].astype(jnp.float32)
    sums[...] = total
    ysend[...] = sums[give, :].astype(jnp.bfloat16)
    y_sum = copy(RSY, ysend, yrecv, far)
    y_sum.start()
    p1.wait_recv()
    correlate(0, 4 * rows, prows + prows // 2, prows // 2, c1, 0)

    @pl.loop(0, nga - 1)
    def _(k):
        at, device = other(k)
        copy(RS1, c1.at[at], r1.at[mine], device).start()

    r1[mine, :] = c1[mine, :]

    y_sum.wait_recv()
    for b in range(CUTS[0][1] // 128):
        at = pl.ds(b * 128, 128)
        dall[mine, at] = couple(sums[keep, at] + yrecv[:, at].astype(jnp.float32), b)

    @pl.loop(0, npeers - 1)
    def _(k):
        _, device = other(2 * k + 1)
        copy(AG0, dall.at[mine, first], dall.at[mine, first], device).start()

    all_rs1.wait_recv()
    total = r1[pl.ds(0, piece), :].astype(jnp.float32)
    for q in range(1, nga):
        total += r1[pl.ds(q * piece, piece), :].astype(jnp.float32)
    dall[mine, last] = couple(total, 3)

    @pl.loop(0, nga - 1)
    def _(k):
        _, device = other(k)
        copy(AG1, dall.at[mine, last], dall.at[mine, last], device).start()

    all_ag0.wait_recv()
    half_block = pl.ds(pl.multiple_of(core * 2 * rows, 2 * rows), 2 * rows)
    to_twin = copy(AGC, dall.at[half_block, first], dall.at[half_block, first], twin)
    to_twin.start()
    to_twin.wait_recv()
    all_ag1.wait_recv()

    quarter = half // 2

    def send_part(index, sub, device):
        slot = (index - T2A) // 2
        at = pl.ds(sub * quarter, quarter)
        return copy(
            index + sub, part_send.at[slot, :, at], part_recv.at[slot, :, at], device
        )

    def partial(block, side, sub):
        return jnp.dot(
            dall[pl.ds(block * rows, rows), :],
            pbuf[:, pl.ds(side * half + sub * quarter, quarter)],
            preferred_element_type=jnp.float32,
        )

    def put(index, sub, value):
        part_send[(index - T2A) // 2, :, pl.ds(sub * quarter, quarter)] = value.astype(
            jnp.bfloat16
        )

    def got(index, sub):
        return part_recv[(index - T2A) // 2, :, pl.ds(sub * quarter, quarter)].astype(
            jnp.float32
        )

    targets = {T2A: right, RB: right, ACA: right, T2B: left, LA: left, ACB: left}
    parts = {(i, sub): send_part(i, sub, targets[i]) for i in targets for sub in range(2)}
    for index, index2, block, block2 in ((T2A, T2B, 3, 3), (RB, LA, 2, 1)):
        for sub in range(2):
            put(index, sub, partial(block, 0 if index == T2A else 1, sub))
            parts[index, sub].start()
            put(index2, sub, partial(block2, 1 if index2 == T2B else 0, sub))
            parts[index2, sub].start()
    at_a = [pl.ds(sub * quarter, quarter) for sub in range(2)]
    at_b = [pl.ds(half + sub * quarter, quarter) for sub in range(2)]
    for sub in range(2):
        own[:, at_a[sub]] = partial(2, 0, sub)
        own[:, at_b[sub]] = partial(1, 1, sub)
    for sub in range(2):
        parts[T2A, sub].wait_recv()
        put(ACA, sub, own[:, at_a[sub]] + got(T2A, sub))
        parts[ACA, sub].start()
        parts[T2B, sub].wait_recv()
        put(ACB, sub, own[:, at_b[sub]] + got(T2B, sub))
        parts[ACB, sub].start()
    load_kin.wait()
    for side, at in enumerate((at_a, at_b)):
        for sub in range(2):
            own[:, at[sub]] = partial(0, side, sub) + kin_ref[:, at[sub]] * wbuf[
                pl.ds(0, rows), at[sub]
            ].astype(jnp.float32)
    for sub in range(2):
        parts[LA, sub].wait_recv()
        own[:, at_a[sub]] += got(LA, sub)
        parts[RB, sub].wait_recv()
        own[:, at_b[sub]] += got(RB, sub)
    for sub in range(2):
        parts[ACA, sub].wait_recv()
        out_ref[:, at_a[sub]] = (own[:, at_a[sub]] + got(ACA, sub)).astype(jnp.bfloat16)
        parts[ACB, sub].wait_recv()
        out_ref[:, at_b[sub]] = (own[:, at_b[sub]] + got(ACB, sub)).astype(jnp.bfloat16)

    for c in (w0r, w1r, w1l, w0l, fr, fl, p0, p1, y_sum, to_twin, *parts.values()):
        c.wait_send()
    for c in (all_rs0, all_rs1, all_ag0, all_ag1):
        c.wait_send()


def local(wavefunctions, projectors, kinetic_diag, species_index, coupling):
    rows, cols = wavefunctions.shape
    prows = projectors.shape[0]
    width = 2 * prows
    bf16, f32 = jnp.bfloat16, jnp.float32
    share = 4 * rows // (2 * NZ)
    vmem = pl.BlockSpec(memory_space=pltpu.VMEM)
    hbm = pl.BlockSpec(memory_space=pltpu.HBM)
    return pl.pallas_call(
        kernel,
        out_shape=jax.ShapeDtypeStruct((rows, cols), bf16),
        in_specs=[hbm, hbm, hbm, hbm, vmem],
        out_specs=vmem,
        scratch_shapes=[
            pltpu.VMEM((4 * rows, cols), bf16),
            pltpu.VMEM((width, cols), bf16),
            pltpu.VMEM((4 * rows, CUTS[0][1]), bf16),
            pltpu.VMEM((4 * rows, CUTS[1][1]), bf16),
            pltpu.VMEM((4 * rows, CUTS[0][1]), bf16),
            pltpu.VMEM((4 * rows, CUTS[1][1]), bf16),
            pltpu.VMEM((share, CUTS[0][1]), f32),
            pltpu.VMEM((share // 2, CUTS[0][1]), bf16),
            pltpu.VMEM((share // 2, CUTS[0][1]), bf16),
            pltpu.VMEM((4 * rows, width), bf16),
            pltpu.VMEM((6, rows, cols // 2), bf16),
            pltpu.VMEM((6, rows, cols // 2), bf16),
            pltpu.VMEM((rows, cols), f32),
            pltpu.VMEM((width, 128), f32),
            pltpu.VMEM((1, cols), f32),
            pltpu.SMEM(species_index.shape, jnp.int32),
            pltpu.SemaphoreType.DMA((COPIES,)),
            pltpu.SemaphoreType.DMA((COPIES,)),
            pltpu.SemaphoreType.DMA((4,)),
            pltpu.SemaphoreType.REGULAR((ROUNDS + 1,)),
        ],
        compiler_params=pltpu.CompilerParams(
            collective_id=0, has_side_effects=True, vmem_limit_bytes=67043328
        ),
    )(wavefunctions, projectors, kinetic_diag.reshape(1, cols), species_index, coupling)


def solution(mesh):
    in_specs = (P("band", "ga"), P("band", "ga"), P("ga"), P(), P())
    out_specs = P("band", "ga")
    return jax.shard_map(local, mesh=mesh, in_specs=in_specs, out_specs=out_specs, check_vma=False)
```

```python
import jax
import jax.numpy as jnp
from jax import lax
from jax.experimental import pallas as pl
from jax.experimental.pallas import tpu as pltpu
from jax.sharding import PartitionSpec as P

NPA = 8
NX = 4
NZ = 8
MESH = pl.DeviceIdType.MESH
CUTS = ((0, 384), (384, 128))
W0R, W1R, W1L, W0L, FR, FL, P0, P1, RS0, RSY, RS1, AG0, AGC, AG1 = range(14)
T2A, T2B, RB, LA, ACA, ACB = range(14, 26, 2)
COPIES = 26
ROUNDS = 4


def kernel(
    w_hbm,
    p_hbm,
    kin_hbm,
    species_hbm,
    coupling_ref,
    out_ref,
    wbuf,
    pbuf,
    c0,
    c1,
    r0,
    r1,
    sums,
    ysend,
    yrecv,
    dall,
    part_send,
    part_recv,
    own,
    block_diag,
    kin_ref,
    species,
    send_sem,
    recv_sem,
    load_sem,
    meet_sem,
):
    band = lax.axis_index("band")
    ga = lax.axis_index("ga")
    rows, cols = w_hbm.shape
    prows = p_hbm.shape[0]
    half_rows = rows // 2
    half = cols // 2
    x = lax.rem(band, NX)
    y_lo = band // NX
    core = lax.rem(ga, 2)
    y_hi = lax.rem(ga // 2, 2)
    z = ga // 4
    right = (y_lo * NX + lax.rem(x + 1, NX), ga)
    left = (y_lo * NX + lax.rem(x + NX - 1, NX), ga)
    across = ((1 - y_lo) * NX + x, ga)

    def at_place(z, y_hi, core):
        return (band, (z * 2 + y_hi) * 2 + core)

    far = at_place(z, 1 - y_hi, core)
    twin = at_place(z, y_hi, 1 - core)
    above = at_place(lax.rem(z + 1, NZ), y_hi, core)
    below = at_place(lax.rem(z + NZ - 1, NZ), y_hi, core)
    nga = 4 * NZ
    npeers = 2 * NZ
    peer = core * NZ + z

    def copy(index, src, dst, device):
        return pltpu.make_async_remote_copy(
            src_ref=src,
            dst_ref=dst,
            send_sem=send_sem.at[index],
            recv_sem=recv_sem.at[index],
            device_id=device,
            device_id_type=MESH,
        )

    load_w = pltpu.make_async_copy(w_hbm, wbuf.at[pl.ds(0, rows)], load_sem.at[0])
    load_p = pltpu.make_async_copy(p_hbm, pbuf.at[pl.ds(0, prows)], load_sem.at[1])
    load_kin = pltpu.make_async_copy(kin_hbm, kin_ref, load_sem.at[2])
    load_species = pltpu.make_async_copy(species_hbm, species, load_sem.at[3])
    for c in (load_species, load_w, load_p, load_kin):
        c.start()

    barrier = pltpu.get_barrier_semaphore()
    near = (right, left, across, far, twin, above, below)
    for device in near:
        pl.semaphore_signal(barrier, inc=1, device_id=device, device_id_type=MESH)
    pl.semaphore_wait(barrier, len(near))

    wrow = lambda block, part: pl.ds(block * rows + part * half_rows, half_rows)
    phalf = prows // 2
    p0 = copy(P0, pbuf.at[pl.ds(0, phalf)], pbuf.at[pl.ds(prows, phalf)], across)
    p1 = copy(P1, pbuf.at[pl.ds(phalf, phalf)], pbuf.at[pl.ds(prows + phalf, phalf)], across)
    w0r = copy(W0R, wbuf.at[wrow(0, 0)], wbuf.at[wrow(1, 0)], right)
    w1r = copy(W1R, wbuf.at[wrow(0, 1)], wbuf.at[wrow(1, 1)], right)
    w1l = copy(W1L, wbuf.at[wrow(0, 1)], wbuf.at[wrow(2, 1)], left)
    w0l = copy(W0L, wbuf.at[wrow(0, 0)], wbuf.at[wrow(2, 0)], left)
    fr = copy(FR, wbuf.at[wrow(1, 0)], wbuf.at[wrow(3, 0)], right)
    fl = copy(FL, wbuf.at[wrow(2, 1)], wbuf.at[wrow(3, 1)], left)
    load_p.wait()
    p0.start()
    p1.start()
    load_w.wait()
    for c in (w0r, w1l, w1r, w0l):
        c.start()

    load_species.wait()
    lane = lax.broadcasted_iota(jnp.int32, (NPA, 128), 1)
    index_at = lax.broadcasted_iota(jnp.int32, (NPA, 128), 0)
    spread = jnp.where(lax.rem(lane, NPA) == index_at, 1.0, 0.0).astype(jnp.float32)
    turned = [
        lax.dot_general(
            coupling_ref[k],
            spread,
            (((0,), (0,)), ((), ())),
            precision=lax.Precision.HIGHEST,
            preferred_element_type=jnp.float32,
        )
        for k in range(coupling_ref.shape[0])
    ]
    q_at = lax.broadcasted_iota(jnp.int32, (128, 128), 0) // NPA
    p_at = lax.broadcasted_iota(jnp.int32, (128, 128), 1) // NPA
    per_block = 128 // NPA
    atoms = prows // NPA
    for b in range(4):
        first = (band if b < 2 else across[0]) * atoms + (b % 2) * per_block
        kinds = jnp.zeros((NPA, 128), jnp.int32)
        for a in range(per_block):
            kinds = jnp.where(lane // NPA == a, species[first + a], kinds)
        strip = jnp.zeros((NPA, 128), jnp.float32)
        for k, matrix in enumerate(turned):
            strip = jnp.where(kinds == k, matrix, strip)
        tiled = jnp.concatenate([strip] * per_block, axis=0)
        block_diag[pl.ds(b * 128, 128), :] = jnp.where(q_at == p_at, tiled, 0.0)

    for i in range(ROUNDS):
        for device in (above, below):
            pl.semaphore_signal(
                meet_sem.at[i], inc=1, device_id=device, device_id_type=MESH
            )
        pl.semaphore_wait(meet_sem.at[i], 2)
    pl.semaphore_signal(
        meet_sem.at[ROUNDS], inc=1, device_id=twin, device_id_type=MESH
    )
    pl.semaphore_wait(meet_sem.at[ROUNDS], 1)

    def correlate(row, count, pstart, pcount, target, tcol):
        c = lax.dot_general(
            wbuf[pl.ds(row, count), :],
            pbuf[pl.ds(pstart, pcount), :],
            (((1,), (1,)), ((), ())),
            preferred_element_type=jnp.float32,
        )
        target[pl.ds(row, count), pl.ds(tcol, pcount)] = c.astype(jnp.bfloat16)

    share = 4 * rows // npeers
    piece = share // 2
    mine = pl.ds(pl.multiple_of((peer * 2 + y_hi) * piece, piece), piece)
    keep = pl.ds(pl.multiple_of(y_hi * piece, piece), piece)
    give = pl.ds(pl.multiple_of((1 - y_hi) * piece, piece), piece)
    first, last = (pl.ds(*cut) for cut in CUTS)

    def many(index, ref):
        return copy(index, ref, ref, right)

    all_rs0 = many(RS0, r0.at[pl.ds(0, (npeers - 1) * share)])
    all_rs1 = many(RS1, r1.at[pl.ds(0, (nga - 1) * piece)])
    all_ag0 = many(AG0, dall.at[pl.ds(0, (npeers - 1) * piece), first])
    all_ag1 = many(AG1, dall.at[pl.ds(0, (nga - 1) * piece), last])

    def scatter_first(row, count, at):
        low, size = row // share, count // share

        for k in range(size):
            q = low + k

            @pl.when(q != peer)
            def _():
                copy(
                    RS0,
                    c0.at[pl.ds(q * share, share), at],
                    r0.at[pl.ds(pl.multiple_of(peer * share, share), share), at],
                    at_place(q % NZ, y_hi, q // NZ),
                ).start()

    def other(k):
        i = k // 4
        d = NZ // 2 + jnp.where(lax.rem(i, 2) == 0, i // 2, -((i + 1) // 2))
        place = (
            lax.rem(z + d, NZ),
            lax.rem(y_hi + 1 - lax.rem(k, 4) // 2, 2),
            lax.rem(core + 1 - lax.rem(k, 2), 2),
        )
        row = ((place[2] * NZ + place[0]) * 2 + place[1]) * piece
        return pl.ds(pl.multiple_of(row, piece), piece), at_place(*place)

    def couple(total, b):
        return jnp.dot(
            total,
            block_diag[pl.ds(b * 128, 128), :],
            precision=lax.Precision.HIGHEST,
            preferred_element_type=jnp.float32,
        ).astype(jnp.bfloat16)

    begun, added = pl.ds(0, prows), pl.ds(prows, phalf)

    def correlate_first(row, count):
        correlate(row, count, 0, prows, c0, 0)
        scatter_first(row, count, begun)

    correlate_first(0, rows)
    w0r.wait_recv()
    fr.start()
    w1l.wait_recv()
    fl.start()
    correlate_first(rows, half_rows)
    correlate_first(2 * rows + half_rows, half_rows)
    p0.wait_recv()
    correlate(0, rows, prows, phalf, c0, prows)
    scatter_first(0, rows, added)
    w1r.wait_recv()
    w0l.wait_recv()
    correlate_first(rows + half_rows, rows)
    correlate(rows, 2 * rows, prows, phalf, c0, prows)
    scatter_first(rows, 2 * rows, added)
    fr.wait_recv()
    fl.wait_recv()
    correlate(3 * rows, rows, 0, prows + phalf, c0, 0)
    scatter_first(3 * rows, rows, first)
    here = pl.ds(pl.multiple_of(peer * share, share), share)
    r0[here, :] = c0[here, :]

    all_rs0.wait_recv()
    total = r0[pl.ds(0, share), :].astype(jnp.float32)
    for q in range(1, npeers):
        total += r0[pl.ds(q * share, share), :].astype(jnp.float32)
    sums[...] = total
    ysend[...] = sums[give, :].astype(jnp.bfloat16)
    y_sum = copy(RSY, ysend, yrecv, far)
    y_sum.start()
    y_sum.wait_recv()
    for b in range(CUTS[0][1] // 128):
        at = pl.ds(b * 128, 128)
        dall[mine, at] = couple(sums[keep, at] + yrecv[:, at].astype(jnp.float32), b)

    @pl.loop(0, npeers - 1, unroll=True)
    def _(k):
        _, device = other(2 * k + 1)
        copy(AG0, dall.at[mine, first], dall.at[mine, first], device).start()

    p1.wait_recv()
    correlate(0, 4 * rows, prows + prows // 2, prows // 2, c1, 0)

    @pl.loop(0, nga - 1, unroll=True)
    def _(k):
        at, device = other(k)
        copy(RS1, c1.at[at], r1.at[mine], device).start()

    r1[mine, :] = c1[mine, :]

    all_rs1.wait_recv()
    total = r1[pl.ds(0, piece), :].astype(jnp.float32)
    for q in range(1, nga):
        total += r1[pl.ds(q * piece, piece), :].astype(jnp.float32)
    dall[mine, last] = couple(total, 3)

    @pl.loop(0, nga - 1, unroll=True)
    def _(k):
        _, device = other(k)
        copy(AG1, dall.at[mine, last], dall.at[mine, last], device).start()

    all_ag0.wait_recv()
    half_block = pl.ds(pl.multiple_of(core * 2 * rows, 2 * rows), 2 * rows)
    to_twin = copy(AGC, dall.at[half_block, first], dall.at[half_block, first], twin)
    to_twin.start()
    to_twin.wait_recv()
    all_ag1.wait_recv()

    quarter = half // 2

    def send_part(index, sub, device):
        slot = (index - T2A) // 2
        at = pl.ds(sub * quarter, quarter)
        return copy(
            index + sub, part_send.at[slot, :, at], part_recv.at[slot, :, at], device
        )

    def partial(block, side, sub):
        return jnp.dot(
            dall[pl.ds(block * rows, rows), :],
            pbuf[:, pl.ds(side * half + sub * quarter, quarter)],
            preferred_element_type=jnp.float32,
        )

    def put(index, sub, value):
        part_send[(index - T2A) // 2, :, pl.ds(sub * quarter, quarter)] = value.astype(
            jnp.bfloat16
        )

    def got(index, sub):
        return part_recv[(index - T2A) // 2, :, pl.ds(sub * quarter, quarter)].astype(
            jnp.float32
        )

    targets = {T2A: right, RB: right, ACA: right, T2B: left, LA: left, ACB: left}
    parts = {(i, sub): send_part(i, sub, targets[i]) for i in targets for sub in range(2)}
    for index, index2, block, block2 in ((T2A, T2B, 3, 3), (RB, LA, 2, 1)):
        for sub in range(2):
            put(index, sub, partial(block, 0 if index == T2A else 1, sub))
            parts[index, sub].start()
            put(index2, sub, partial(block2, 1 if index2 == T2B else 0, sub))
            parts[index2, sub].start()
    at_a = [pl.ds(sub * quarter, quarter) for sub in range(2)]
    at_b = [pl.ds(half + sub * quarter, quarter) for sub in range(2)]
    for sub in range(2):
        own[:, at_a[sub]] = partial(2, 0, sub)
        own[:, at_b[sub]] = partial(1, 1, sub)
    for sub in range(2):
        parts[T2A, sub].wait_recv()
        put(ACA, sub, own[:, at_a[sub]] + got(T2A, sub))
        parts[ACA, sub].start()
        parts[T2B, sub].wait_recv()
        put(ACB, sub, own[:, at_b[sub]] + got(T2B, sub))
        parts[ACB, sub].start()
    load_kin.wait()
    for side, at in enumerate((at_a, at_b)):
        for sub in range(2):
            own[:, at[sub]] = partial(0, side, sub) + kin_ref[:, at[sub]] * wbuf[
                pl.ds(0, rows), at[sub]
            ].astype(jnp.float32)
    for sub in range(2):
        parts[LA, sub].wait_recv()
        own[:, at_a[sub]] += got(LA, sub)
        parts[RB, sub].wait_recv()
        own[:, at_b[sub]] += got(RB, sub)
    for sub in range(2):
        parts[ACA, sub].wait_recv()
        out_ref[:, at_a[sub]] = (own[:, at_a[sub]] + got(ACA, sub)).astype(jnp.bfloat16)
        parts[ACB, sub].wait_recv()
        out_ref[:, at_b[sub]] = (own[:, at_b[sub]] + got(ACB, sub)).astype(jnp.bfloat16)

    for c in (w0r, w1r, w1l, w0l, fr, fl, p0, p1, y_sum, to_twin, *parts.values()):
        c.wait_send()
    for c in (all_rs0, all_rs1, all_ag0, all_ag1):
        c.wait_send()


def local(wavefunctions, projectors, kinetic_diag, species_index, coupling):
    rows, cols = wavefunctions.shape
    prows = projectors.shape[0]
    width = 2 * prows
    bf16, f32 = jnp.bfloat16, jnp.float32
    share = 4 * rows // (2 * NZ)
    vmem = pl.BlockSpec(memory_space=pltpu.VMEM)
    hbm = pl.BlockSpec(memory_space=pltpu.HBM)
    return pl.pallas_call(
        kernel,
        out_shape=jax.ShapeDtypeStruct((rows, cols), bf16),
        in_specs=[hbm, hbm, hbm, hbm, vmem],
        out_specs=vmem,
        scratch_shapes=[
            pltpu.VMEM((4 * rows, cols), bf16),
            pltpu.VMEM((width, cols), bf16),
            pltpu.VMEM((4 * rows, CUTS[0][1]), bf16),
            pltpu.VMEM((4 * rows, CUTS[1][1]), bf16),
            pltpu.VMEM((4 * rows, CUTS[0][1]), bf16),
            pltpu.VMEM((4 * rows, CUTS[1][1]), bf16),
            pltpu.VMEM((share, CUTS[0][1]), f32),
            pltpu.VMEM((share // 2, CUTS[0][1]), bf16),
            pltpu.VMEM((share // 2, CUTS[0][1]), bf16),
            pltpu.VMEM((4 * rows, width), bf16),
            pltpu.VMEM((6, rows, cols // 2), bf16),
            pltpu.VMEM((6, rows, cols // 2), bf16),
            pltpu.VMEM((rows, cols), f32),
            pltpu.VMEM((width, 128), f32),
            pltpu.VMEM((1, cols), f32),
            pltpu.SMEM(species_index.shape, jnp.int32),
            pltpu.SemaphoreType.DMA((COPIES,)),
            pltpu.SemaphoreType.DMA((COPIES,)),
            pltpu.SemaphoreType.DMA((4,)),
            pltpu.SemaphoreType.REGULAR((ROUNDS + 1,)),
        ],
        compiler_params=pltpu.CompilerParams(
            collective_id=0, has_side_effects=True, vmem_limit_bytes=67043328
        ),
    )(wavefunctions, projectors, kinetic_diag.reshape(1, cols), species_index, coupling)


def solution(mesh):
    in_specs = (P("band", "ga"), P("band", "ga"), P("ga"), P(), P())
    out_specs = P("band", "ga")
    return jax.shard_map(local, mesh=mesh, in_specs=in_specs, out_specs=out_specs, check_vma=False)
```
